8 devices in a mesh: prob: 2 (over z, y), feat: 4 (over x, core).
Axes of the slice: x: 2, y: 2, z: 1, core: 2. Of those that a mesh axis runs over, the one named last changes fastest.
Arguments:
- design: bfloat16 [16384, 16384], P(None, ('prob', 'feat')), parts along dimension 1
- w_init: float32 [16384, 101], P(('prob', 'feat')), parts along dimension 0
- targets: float32 [32768, 101], P('prob'), parts along dimension 0
Outputs:
- output 1: float32 [16384, 101], P(('prob', 'feat')), parts along dimension 0
- output 2: float32 [32768, 101], P('prob'), parts along dimension 0
There are 2 independent parts. The reference program is written for one: setup_inputs(seed, part) draws one part's arguments, and reference() takes and returns one part's arrays. A program takes and returns all parts, laid end to end along the dimension named above; each array names one.
All inputs are finite; a program needn't handle non-finite values.
Results may differ from the reference program's by a relative error of at most 0.0043035.
Values are sent between devices in bfloat16 or wider.
A program may use at most 1 GiB of HBM per device.

```python
import math
import jax
import jax.numpy as jnp
from jax import lax

SAMPLES = 16384
TARGETS = 101
FEAT_DEV = 2048
SWEEPS = 6
GROUP = 4
LATENT = 8
LOCAL_STEPS = 2
FEATURES = FEAT_DEV * GROUP
RIDGE = 0.01
GAMMA = 0.75


def latent_scales():
    ratios = 0.6 ** jnp.arange(LATENT, dtype=jnp.float32)
    return ratios * jnp.sqrt(0.5 / jnp.sum(ratios * ratios))


def setup_inputs(seed: int = 0, part: int = 0) -> dict:
    base_key = jax.random.fold_in(jax.random.key(seed), part)
    key_z, key_a, key_e, key_c, key_y, key_w = jax.random.split(base_key, 6)
    scales = latent_scales()
    latent = jax.random.normal(key_z, (SAMPLES, LATENT), jnp.float32)
    loadings = jax.random.normal(key_a, (LATENT, FEATURES), jnp.float32)
    noise = jax.random.normal(key_e, (SAMPLES, FEATURES), jnp.float32)
    design = (jnp.dot(latent * scales, loadings) + math.sqrt(0.5) * noise).astype(jnp.bfloat16)
    coupling = jax.random.normal(key_c, (LATENT, TARGETS), jnp.float32)
    lat_norm = LATENT ** -0.5
    target_noise = jax.random.normal(key_y, (SAMPLES, TARGETS), jnp.float32)
    targets = jnp.dot(latent, coupling) * lat_norm + 0.5 * target_noise
    w_init = jax.random.normal(key_w, (FEATURES, TARGETS), jnp.float32) * (FEATURES ** -0.5)
    return {'design': design, 'w_init': w_init, 'targets': targets}


def block_product(x_block, coef_block):
    full = jnp.dot(x_block, coef_block.astype(jnp.bfloat16), preferred_element_type=jnp.float32)
    return full.astype(jnp.bfloat16).astype(jnp.float32)


def left_product(x_block, resid_part):
    return jnp.dot(x_block.T, resid_part.astype(jnp.bfloat16), preferred_element_type=jnp.float32) / SAMPLES


def block_step(x_block):
    squares = jnp.square(x_block.astype(jnp.float32))
    return SAMPLES / (GROUP * jnp.sum(squares))


def local_passes(x_block, w_block, residual):
    step_size = block_step(x_block)
    gradient = left_product(x_block, residual)
    coef_step = step_size * (gradient - RIDGE * w_block)
    update = block_product(x_block, coef_step)
    for step_idx in range(1, LOCAL_STEPS):
        gradient = left_product(x_block, residual - GROUP * update)
        coef_step = coef_step + step_size * (gradient - RIDGE * (w_block + coef_step))
        update = block_product(x_block, coef_step)
    return coef_step, update


def reference(design, w_init, targets):
    zero_rows = jnp.zeros((SAMPLES, TARGETS), jnp.float32)

    def init_body(total, index):
        x_block = lax.dynamic_slice_in_dim(design, index * FEAT_DEV, FEAT_DEV, axis=1)
        w_block = lax.dynamic_slice_in_dim(w_init, index * FEAT_DEV, FEAT_DEV, axis=0)
        return total + block_product(x_block, w_block), None

    prediction, _ = lax.scan(init_body, zero_rows, jnp.arange(GROUP))

    def sweep_body(carry, unused):
        weights, residual = carry

        def block_body(total, index):
            x_block = lax.dynamic_slice_in_dim(design, index * FEAT_DEV, FEAT_DEV, axis=1)
            w_block = lax.dynamic_slice_in_dim(weights, index * FEAT_DEV, FEAT_DEV, axis=0)
            coef_step, update = local_passes(x_block, w_block, residual)
            return total + update, coef_step

        summed, steps_all = lax.scan(block_body, zero_rows, jnp.arange(GROUP))
        weights = weights + GAMMA * steps_all.reshape(FEATURES, TARGETS)
        residual = residual - GAMMA * summed
        return (weights, residual), None

    (weights, residual), _ = lax.scan(sweep_body, (w_init, targets - prediction), None, length=SWEEPS)
    return weights, residual
```

```python
import functools

import jax
import jax.numpy as jnp
from jax import lax
from jax.experimental import pallas as pl
from jax.experimental.pallas import tpu as pltpu
from jax.sharding import PartitionSpec as P

LOCAL_STEPS = 2
SWEEPS = 6
RIDGE = 0.01
GAMMA = 0.75

MESH = pl.DeviceIdType.MESH
F32 = jnp.float32
BF16 = jnp.bfloat16
ROWS = 104
CHUNK = 512
RING = 8
BLOCK = 512
SIB, CROSS, DIAG = 0, 1, 2


def dot(a, b, dims=((1,), (0,))):
    return lax.dot_general(a, b, (dims, ((), ())), preferred_element_type=F32)


def kernel(samples, group, x_hbm, w0_ref, y_ref, w_ref, r_hbm,
           xbuf, xt, gram, gram_hi, gram_lo, eta_ref, coef, grad, r_own, r_all, u_mine, u_out, u_in,
           x_sem, u_send, u_recv, r_send, r_recv, o_send, o_recv, o_local):
    prob, me = lax.axis_index("prob"), lax.axis_index("feat")
    odd, half = lax.rem(me, 2), me // 2
    sib = half * 2 + (1 - odd)
    cross = (1 - half) * 2 + odd
    diag = (1 - half) * 2 + (1 - odd)
    partner = {SIB: sib, CROSS: cross, DIAG: diag}
    features = x_hbm.shape[1]
    quarter = samples // group
    steps = quarter // CHUNK
    blocks = features // BLOCK

    def device(index):
        return dict(device_id=(prob, index), device_id_type=MESH)

    barrier = pltpu.get_barrier_semaphore()
    for index in (sib, cross, diag):
        pl.semaphore_signal(barrier, inc=1, **device(index))

    def cols(c):
        return pl.ds(pl.multiple_of(c * CHUNK, CHUNK), CHUNK)

    def load(q, c, slot):
        rows = pl.ds(pl.multiple_of(q * quarter + c * CHUNK, CHUNK), CHUNK)
        return pltpu.make_async_copy(x_hbm.at[rows], xbuf.at[slot], x_sem.at[slot])

    a_order = (cross, diag, sib, me)
    b_order = (me, sib)
    c_order = (cross, diag)
    per = {"a": RING // 4, "b": RING // 2, "c": RING // 2}
    orders = {"a": a_order, "b": b_order, "c": c_order}

    def prefetch(phase, c, i, slot):
        if phase == "gram":
            load(0, c, slot).start()
        elif phase is not None:
            load(orders[phase][i], c, slot).start()

    def rounds(phase, nxt, body):
        n, order = per[phase], orders[phase]
        width = len(order)

        def run(c, ahead):
            for i in range(width):
                slot = lax.rem(c * width + i, RING)
                load(order[i], c, slot).wait()
                body(c, i, order[i], xbuf.at[slot])
                ahead(c, i, slot)

        def main(c, carry):
            run(c, lambda c, i, slot: prefetch(phase, c + n, i, slot))
            return carry

        def tail(c, carry):
            def ahead(c, i, slot):
                if nxt is None:
                    return
                k = (c - (steps - n)) * width + i
                if nxt == "gram":
                    prefetch(nxt, k, 0, slot)
                elif len(orders[nxt]) == width:
                    prefetch(nxt, c - (steps - n), i, slot)
                elif width == 4:
                    prefetch(nxt, (c - (steps - n)) * 2 + i // 2, i % 2, slot)
                else:
                    j = lax.rem(c - (steps - n), 2)
                    lo, hi = orders[nxt][i], orders[nxt][2 + i]
                    load(lo + j * (hi - lo), (c - (steps - n)) // 2, slot).start()
            run(c, ahead)
            return carry

        lax.fori_loop(0, steps - n, main, 0)
        lax.fori_loop(steps - n, steps, tail, 0)

    def u_copy(rel, c):
        return pltpu.make_async_remote_copy(
            u_out.at[rel, :, cols(c)], u_in.at[rel, :, cols(c)],
            u_send.at[rel, c], u_recv.at[rel, c], **device(partner[rel]))

    def r_copy(rel, c, q, target):
        return pltpu.make_async_remote_copy(
            r_all.at[q, :, cols(c)], r_all.at[q, :, cols(c)],
            r_send.at[rel, c], r_recv.at[rel, c], **device(target))

    a_rel = (CROSS, DIAG, SIB, None)

    def phase_a(nxt):
        def body(c, i, q, x):
            u = dot(coef[...], x[...], ((1,), (1,))).astype(BF16)
            if a_rel[i] is None:
                u_mine[:, cols(c)] = u
            else:
                u_out[a_rel[i], :, cols(c)] = u
                u_copy(a_rel[i], c).start()
        rounds("a", nxt, body)

    def residual(c, factor):
        for rel in (SIB, CROSS, DIAG):
            u_copy(rel, c).wait_recv()
        total = u_mine[:, cols(c)].astype(F32)
        for rel in (SIB, CROSS, DIAG):
            total = total + u_in[rel, :, cols(c)].astype(F32)
        new = r_own[:, cols(c)] - factor * total
        r_own[:, cols(c)] = new
        return new

    def update(c, factor):
        r_all[me, :, cols(c)] = residual(c, factor).astype(BF16)
        r_copy(CROSS, c, me, cross).start()
        r_copy(SIB, c, me, sib).start()

    def accumulate(c, q, x):
        grad[...] += dot(r_all[q, :, cols(c)], x[...])

    def phase_b(factor):
        def body(c, i, q, x):
            if i == 0:
                if factor is not None:
                    update(c, factor)
            else:
                r_copy(SIB, c, sib, sib).wait_recv()
            accumulate(c, q, x)
        grad[...] = jnp.zeros_like(grad)
        rounds("b", "c", body)

    def phase_c():
        def body(c, i, q, x):
            if i == 0:
                r_copy(CROSS, c, cross, cross).wait_recv()
                r_copy(DIAG, c, cross, sib).start()
            else:
                r_copy(DIAG, c, diag, sib).wait_recv()
            accumulate(c, q, x)
        rounds("c", "a", body)

    def wait_u(c, carry):
        for rel in (SIB, CROSS, DIAG):
            u_copy(rel, c).wait_send()
        return carry

    def wait_r(c, carry):
        r_copy(CROSS, c, me, cross).wait_send()
        r_copy(SIB, c, me, sib).wait_send()
        r_copy(DIAG, c, cross, sib).wait_send()
        return carry

    def local_passes():
        eta = eta_ref[...]
        weights = w_ref[...]
        first = eta * (grad[...] * (1.0 / samples) - RIDGE * weights)
        lhs = first.astype(BF16)
        curved = dot(lhs, gram_hi[...]) + dot(lhs, gram_lo[...])
        curved = jnp.where(eta > 0, curved, 0.0)
        gradient = (grad[...] - (4.0 * group) * curved) * (1.0 / samples)
        second = first + eta * (gradient - RIDGE * (weights + first))
        w_ref[...] = weights + GAMMA * second
        coef[...] = second.astype(BF16)

    def block_index(i, j):
        return i * (i + 1) // 2 + j

    def gram_steps(start, stop, ahead):
        def step(k, carry):
            slot = lax.rem(k, RING)
            load(0, k, slot).wait()
            xt[...] = xbuf[slot].T
            for i in range(blocks):
                for j in range(i + 1):
                    left = xt[i * BLOCK:(i + 1) * BLOCK, :]
                    right = xbuf[slot, :, j * BLOCK:(j + 1) * BLOCK]
                    gram[block_index(i, j)] += dot(left, right)
            ahead(k, slot)
            return carry
        lax.fori_loop(start, stop, step, 0)

    def gram_finish():
        trace = jnp.zeros((1, 1), F32)
        for i in range(blocks):
            for j in range(i + 1):
                block = gram[block_index(i, j)]
                if i == j:
                    row = lax.broadcasted_iota(jnp.int32, block.shape, 0)
                    col = lax.broadcasted_iota(jnp.int32, block.shape, 1)
                    picked = jnp.where(row == col, block, 0.0)
                    trace = trace + jnp.sum(jnp.sum(picked, axis=0, keepdims=True), axis=1, keepdims=True)
                scaled = block * 0.25
                rows, columns = slice(i * BLOCK, (i + 1) * BLOCK), slice(j * BLOCK, (j + 1) * BLOCK)
                high = scaled.astype(BF16)
                gram_hi[rows, columns] = high
                gram_lo[rows, columns] = (scaled - high.astype(F32)).astype(BF16)
                if i != j:
                    scaled = scaled.T
                    high = scaled.astype(BF16)
                    gram_hi[columns, rows] = high
                    gram_lo[columns, rows] = (scaled - high.astype(F32)).astype(BF16)
        eta_ref[...] = jnp.broadcast_to(samples / (group * trace), eta_ref.shape)

    for k in range(RING):
        load(a_order[k % 4], k // 4, k).start()
    coef[...] = w0_ref[...].astype(BF16)
    w_ref[...] = w0_ref[...]
    r_own[...] = y_ref[...]
    gram[...] = jnp.zeros_like(gram)
    pl.semaphore_wait(barrier, 3)
    phase_a("gram")
    total_steps = samples // CHUNK
    gram_steps(0, total_steps // 2, lambda k, slot: load(0, k + RING, slot).start())

    def first_update(c, carry):
        update(c, 1.0)
        return carry

    lax.fori_loop(0, steps, first_update, 0)
    gram_steps(total_steps // 2, total_steps - RING, lambda k, slot: load(0, k + RING, slot).start())

    def to_b(k, slot):
        j = k - (total_steps - RING)
        load(me + lax.rem(j, 2) * (sib - me), j // 2, slot).start()

    gram_steps(total_steps - RING, total_steps, to_b)
    gram_finish()
    lax.fori_loop(0, steps, wait_u, 0)
    phase_b(None)
    phase_c()
    lax.fori_loop(0, steps, wait_r, 0)
    local_passes()

    def sweep(t, carry):
        phase_a("b")
        phase_b(GAMMA)
        phase_c()
        lax.fori_loop(0, steps, wait_u, 0)
        lax.fori_loop(0, steps, wait_r, 0)
        local_passes()
        return carry

    lax.fori_loop(0, SWEEPS - 1, sweep, 0)

    phase_a(None)

    def o_copy(rel, c, q, target, source):
        return pltpu.make_async_remote_copy(
            source, r_hbm.at[q, :, cols(c)], o_send.at[rel, c], o_recv.at[rel, c], **device(target))

    def o_keep(c):
        return pltpu.make_async_copy(r_own.at[:, cols(c)], r_hbm.at[me, :, cols(c)], o_local.at[c])

    def finish(c, carry):
        residual(c, GAMMA)
        o_copy(CROSS, c, me, cross, r_own.at[:, cols(c)]).start()
        o_copy(SIB, c, me, sib, r_own.at[:, cols(c)]).start()
        o_keep(c).start()
        return carry

    def relay(c, carry):
        o_copy(CROSS, c, cross, cross, r_own.at[:, cols(c)]).wait_recv()
        o_copy(DIAG, c, cross, sib, r_hbm.at[cross, :, cols(c)]).start()
        return carry

    def drain(c, carry):
        o_copy(SIB, c, sib, sib, r_own.at[:, cols(c)]).wait_recv()
        o_copy(DIAG, c, diag, sib, r_own.at[:, cols(c)]).wait_recv()
        for rel, target in ((CROSS, cross), (SIB, sib)):
            o_copy(rel, c, me, target, r_own.at[:, cols(c)]).wait_send()
        o_copy(DIAG, c, cross, sib, r_hbm.at[cross, :, cols(c)]).wait_send()
        o_keep(c).wait()
        return carry

    lax.fori_loop(0, steps, finish, 0)
    lax.fori_loop(0, steps, relay, 0)
    lax.fori_loop(0, steps, wait_u, 0)
    lax.fori_loop(0, steps, drain, 0)


def solution(mesh):
    group = mesh.shape['feat']

    def per_device(design, w_init, targets):
        samples, features = design.shape
        labels = w_init.shape[1]
        quarter = samples // group
        steps = quarter // CHUNK
        blocks = features // BLOCK
        pad = ((0, ROWS - labels), (0, 0))
        own = lax.dynamic_slice_in_dim(targets, lax.axis_index('feat') * quarter, quarter, 0)
        w_t = jnp.pad(w_init.T, pad)
        y_t = jnp.pad(own.T, pad)
        vmem = pl.BlockSpec(memory_space=pltpu.VMEM)
        anywhere = pl.BlockSpec(memory_space=pl.ANY)
        dma = pltpu.SemaphoreType.DMA
        weights, residual = pl.pallas_call(
            functools.partial(kernel, samples, group),
            out_shape=(jax.ShapeDtypeStruct((ROWS, features), F32),
                       jax.ShapeDtypeStruct((group, ROWS, quarter), F32)),
            in_specs=[anywhere, vmem, vmem],
            out_specs=(vmem, anywhere),
            scratch_shapes=[
                pltpu.VMEM((RING, CHUNK, features), BF16),
                pltpu.VMEM((features, CHUNK), BF16),
                pltpu.VMEM((blocks * (blocks + 1) // 2, BLOCK, BLOCK), F32),
                pltpu.VMEM((features, features), BF16),
                pltpu.VMEM((features, features), BF16),
                pltpu.VMEM((1, features), F32),
                pltpu.VMEM((ROWS, features), BF16),
                pltpu.VMEM((ROWS, features), F32),
                pltpu.VMEM((ROWS, quarter), F32),
                pltpu.VMEM((group, ROWS, quarter), BF16),
                pltpu.VMEM((ROWS, quarter), BF16),
                pltpu.VMEM((3, ROWS, quarter), BF16),
                pltpu.VMEM((3, ROWS, quarter), BF16),
                dma((RING,)),
                dma((3, steps)), dma((3, steps)),
                dma((3, steps)), dma((3, steps)),
                dma((3, steps)), dma((3, steps)),
                dma((steps,)),
            ],
            compiler_params=pltpu.CompilerParams(
                collective_id=0, has_side_effects=True, vmem_limit_bytes=67000000),
        )(design, w_t, y_t)
        residual = residual.transpose(0, 2, 1).reshape(samples, ROWS)[:, :labels]
        return weights.T[:, :labels], residual

    return jax.shard_map(
        per_device,
        mesh=mesh,
        in_specs=(P(None, ('prob', 'feat')), P(('prob', 'feat'), None), P('prob', None)),
        out_specs=(P(('prob', 'feat'), None), P('prob', None)),
        check_vma=False,
    )
```

```python
import functools

import jax
import jax.numpy as jnp
from jax import lax
from jax.experimental import pallas as pl
from jax.experimental.pallas import tpu as pltpu
from jax.sharding import PartitionSpec as P

LOCAL_STEPS = 2
SWEEPS = 6
RIDGE = 0.01
GAMMA = 0.75

MESH = pl.DeviceIdType.MESH
F32 = jnp.float32
BF16 = jnp.bfloat16
CHUNK = 512
RING = 8
BLOCK = 512
HALF = BLOCK // 2
SIB, CROSS, DIAG = 0, 1, 2


def dot(a, b, dims=((1,), (0,))):
    return lax.dot_general(a, b, (dims, ((), ())), preferred_element_type=F32)


def kernel(samples, group, x_hbm, w0_hbm, y_hbm, w_ref, r_hbm,
           xbuf, xt0, xt1, gram, gram_hi, gram_lo, eta_ref, coef, grad, r_own, r_all, u_mine, u_out, u_in,
           x_sem, u_send, u_recv, r_send, r_recv, o_send, o_recv, o_local, in_sem):
    prob, me = lax.axis_index("prob"), lax.axis_index("feat")
    odd, half = lax.rem(me, 2), me // 2
    sib = half * 2 + (1 - odd)
    cross = (1 - half) * 2 + odd
    diag = (1 - half) * 2 + (1 - odd)
    partner = {SIB: sib, CROSS: cross, DIAG: diag}
    features = x_hbm.shape[1]
    quarter = samples // group
    steps = quarter // CHUNK
    blocks = features // BLOCK

    def device(index):
        return dict(device_id=(prob, index), device_id_type=MESH)

    barrier = pltpu.get_barrier_semaphore()
    for index in (sib, cross, diag):
        pl.semaphore_signal(barrier, inc=1, **device(index))

    def cols(c):
        return pl.ds(pl.multiple_of(c * CHUNK, CHUNK), CHUNK)

    def load(q, c, slot):
        rows = pl.ds(pl.multiple_of(q * quarter + c * CHUNK, CHUNK), CHUNK)
        return pltpu.make_async_copy(x_hbm.at[rows], xbuf.at[slot], x_sem.at[slot])

    a_order = (cross, diag, sib, me)
    b_order = (me, sib)
    c_order = (cross, diag)
    per = {"a": RING // 4, "b": RING // 2, "c": RING // 2}
    orders = {"a": a_order, "b": b_order, "c": c_order}

    def prefetch(phase, c, i, slot):
        load(orders[phase][i], c, slot).start()

    def rounds(phase, nxt, body, together=1):
        n, order = per[phase], orders[phase]
        width = len(order)

        def run(c, ahead):
            for first in range(0, width, together):
                some = range(first, first + together)
                slots = [lax.rem(c * width + i, RING) for i in some]
                for i, slot in zip(some, slots):
                    load(order[i], c, slot).wait()
                sends = [body(c, i, order[i], xbuf.at[slot]) for i, slot in zip(some, slots)]
                for i, slot, send in zip(some, slots, sends):
                    if send is not None:
                        send.start()
                    ahead(c, i, slot)

        def main(c, carry):
            run(c, lambda c, i, slot: prefetch(phase, c + n, i, slot))
            return carry

        def tail(c, carry):
            def ahead(c, i, slot):
                if nxt is None:
                    return
                k = (c - (steps - n)) * width + i
                if nxt == "start":
                    load(diag, k, slot).start()
                elif len(orders[nxt]) == width:
                    prefetch(nxt, c - (steps - n), i, slot)
                elif width == 4:
                    prefetch(nxt, (c - (steps - n)) * 2 + i // 2, i % 2, slot)
                else:
                    j = lax.rem(c - (steps - n), 2)
                    lo, hi = orders[nxt][i], orders[nxt][2 + i]
                    load(lo + j * (hi - lo), (c - (steps - n)) // 2, slot).start()
            run(c, ahead)
            return carry

        lax.fori_loop(0, steps - n, main, 0)
        lax.fori_loop(steps - n, steps, tail, 0)

    def u_copy(rel, c):
        return pltpu.make_async_remote_copy(
            u_out.at[rel, :, cols(c)], u_in.at[rel, :, cols(c)],
            u_send.at[rel, c], u_recv.at[rel, c], **device(partner[rel]))

    def r_copy(rel, c, q, target):
        return pltpu.make_async_remote_copy(
            r_all.at[q, :, cols(c)], r_all.at[q, :, cols(c)],
            r_send.at[rel, c], r_recv.at[rel, c], **device(target))

    a_rel = (CROSS, DIAG, SIB, None)

    def phase_a(nxt, together=1):
        def body(c, i, q, x):
            u = dot(coef[...], x[...], ((1,), (1,))).astype(BF16)
            if a_rel[i] is None:
                u_mine[:, cols(c)] = u
                return None
            u_out[a_rel[i], :, cols(c)] = u
            return u_copy(a_rel[i], c)
        rounds("a", nxt, body, together)

    def residual(c, factor):
        for rel in (SIB, CROSS, DIAG):
            u_copy(rel, c).wait_recv()
        total = u_mine[:, cols(c)].astype(F32)
        for rel in (SIB, CROSS, DIAG):
            total = total + u_in[rel, :, cols(c)].astype(F32)
        new = r_own[:, cols(c)] - factor * total
        r_own[:, cols(c)] = new
        return new

    def update(c, factor):
        r_all[me, :, cols(c)] = residual(c, factor).astype(BF16)
        r_copy(CROSS, c, me, cross).start()
        r_copy(SIB, c, me, sib).start()

    def accumulate(c, q, x):
        grad[...] += dot(r_all[q, :, cols(c)], x[...])

    def phase_b():
        def body(c, i, q, x):
            if i == 0:
                update(c, GAMMA)
            else:
                r_copy(SIB, c, sib, sib).wait_recv()
            accumulate(c, q, x)
        grad[...] = jnp.zeros_like(grad)
        rounds("b", "c", body)

    def phase_c():
        def body(c, i, q, x):
            if i == 0:
                r_copy(CROSS, c, cross, cross).wait_recv()
                r_copy(DIAG, c, cross, sib).start()
            else:
                r_copy(DIAG, c, diag, sib).wait_recv()
            accumulate(c, q, x)
        rounds("c", "a", body)

    def wait_u(c, carry):
        for rel in (SIB, CROSS, DIAG):
            u_copy(rel, c).wait_send()
        return carry

    def wait_r(c, carry):
        r_copy(CROSS, c, me, cross).wait_send()
        r_copy(SIB, c, me, sib).wait_send()
        return carry

    def wait_relay(c, carry):
        r_copy(DIAG, c, cross, sib).wait_send()
        return carry

    def local_passes():
        eta = eta_ref[...]
        weights = w_ref[...]
        first = eta * (grad[...] * (1.0 / samples) - RIDGE * weights)
        lhs = first.astype(BF16)
        curved = dot(lhs, gram_hi[...]) + dot(lhs, gram_lo[...])
        curved = jnp.where(eta > 0, curved, 0.0)
        gradient = (grad[...] - (4.0 * group) * curved) * (1.0 / samples)
        second = first + eta * (gradient - RIDGE * (weights + first))
        w_ref[...] = weights + GAMMA * second
        coef[...] = second.astype(BF16)

    def block_index(i, j):
        return i * (i + 1) // 2 + j

    def gram_add(left_ref, right_ref):
        for i in range(blocks):
            for j in range(i + 1):
                left = left_ref[i * BLOCK:(i + 1) * BLOCK, :]
                right = right_ref[:, j * BLOCK:(j + 1) * BLOCK]
                if i == j:
                    gram[block_index(i, j), HALF:, :] += dot(left[HALF:], right)
                    gram[block_index(i, j), :HALF, :HALF] += dot(left[:HALF], right[:, :HALF])
                else:
                    gram[block_index(i, j)] += dot(left, right)

    def start_order(s):
        flip_half, flip_odd = lax.rem(1 + (s + 1) // 2, 2), lax.rem(s + 1, 2)
        return 2 * (half + flip_half * (1 - 2 * half)) + odd + flip_odd * (1 - 2 * odd)

    def start_quarters(first, last, with_gradient):
        def pair(t, carry):
            s, k = t // (steps // 2), lax.rem(t, steps // 2)
            q = start_order(s)
            pairs = ((xt0, xt1), (xt1, xt0))
            for i in range(2):
                c = 2 * k + i
                ahead = lax.rem(c + 1, RING)
                load(q, ahead, ahead).wait()
                if with_gradient:
                    @pl.when(s == 2)
                    def _():
                        r_copy(SIB, c, sib, sib).wait_recv()

                    @pl.when(s == 3)
                    def _():
                        r_copy(CROSS, c, cross, cross).wait_recv()
                        r_copy(DIAG, c, cross, sib).start()
            for i, (now, later) in enumerate(pairs):
                c = 2 * k + i
                later[...] = xbuf[lax.rem(c + 1, RING)].T
                gram_add(now, xbuf.at[c])
                if with_gradient:
                    accumulate(c, q, xbuf.at[c])
            for i in range(2):
                load(start_order(s + 1), 2 * k + i, 2 * k + i).start()
            return carry
        lax.fori_loop(first * (steps // 2), last * (steps // 2), pair, 0)

    def gram_finish():
        trace = jnp.zeros((1, 1), F32)
        for i in range(blocks):
            for j in range(i + 1):
                block = gram[block_index(i, j)]
                if i == j:
                    corner = jnp.concatenate([block[:HALF, :HALF], block[HALF:, :HALF].T], axis=1)
                    block = jnp.concatenate([corner, block[HALF:]], axis=0)
                    row = lax.broadcasted_iota(jnp.int32, block.shape, 0)
                    col = lax.broadcasted_iota(jnp.int32, block.shape, 1)
                    picked = jnp.where(row == col, block, 0.0)
                    trace = trace + jnp.sum(jnp.sum(picked, axis=0, keepdims=True), axis=1, keepdims=True)
                scaled = block * 0.25
                rows, columns = slice(i * BLOCK, (i + 1) * BLOCK), slice(j * BLOCK, (j + 1) * BLOCK)
                high = scaled.astype(BF16)
                gram_hi[rows, columns] = high
                gram_lo[rows, columns] = (scaled - high.astype(F32)).astype(BF16)
                if i != j:
                    scaled = scaled.T
                    high = scaled.astype(BF16)
                    gram_hi[columns, rows] = high
                    gram_lo[columns, rows] = (scaled - high.astype(F32)).astype(BF16)
        eta_ref[...] = jnp.broadcast_to(samples / (group * trace), eta_ref.shape)

    in_w = pltpu.make_async_copy(w0_hbm, w_ref, in_sem.at[0])
    in_y = pltpu.make_async_copy(
        y_hbm.at[:, pl.ds(pl.multiple_of(me * quarter, quarter), quarter)], r_own, in_sem.at[1])
    in_w.start()
    for k in range(RING):
        load(a_order[k % 4], k // 4, k).start()
    in_y.start()
    in_w.wait()
    coef[...] = w_ref[...].astype(BF16)
    pl.semaphore_wait(barrier, 3)
    phase_a("start", 2)
    gram[...] = jnp.zeros_like(gram)
    grad[...] = jnp.zeros_like(grad)
    in_y.wait()

    def first_update(c, carry):
        update(c, 1.0)
        return carry

    load(diag, 0, 0).wait()
    xt0[...] = xbuf[0].T
    start_quarters(0, 1, False)
    lax.fori_loop(0, steps, first_update, 0)
    start_quarters(1, 4, True)
    gram_finish()
    lax.fori_loop(0, steps, wait_u, 0)
    for k in range(steps // 4):
        some = range(4 * k, 4 * k + 4)
        for c in some:
            if c > 0:
                load(diag, c, c).wait()
            r_copy(DIAG, c, diag, sib).wait_recv()
        total = grad[...]
        for c in some:
            total = total + dot(r_all[diag, :, cols(c)], xbuf[c])
        grad[...] = total
        for c in some:
            load(a_order[c % 4], c // 4, c).start()
    lax.fori_loop(0, steps, wait_relay, 0)
    local_passes()

    def sweep(t, carry):
        phase_a("b")
        lax.fori_loop(0, steps, wait_r, 0)
        phase_b()
        lax.fori_loop(0, steps, wait_u, 0)
        phase_c()
        lax.fori_loop(0, steps, wait_relay, 0)
        local_passes()
        return carry

    lax.fori_loop(0, SWEEPS - 1, sweep, 0)

    phase_a(None)
    lax.fori_loop(0, steps, wait_r, 0)

    def out_cols(q, c):
        return pl.ds(pl.multiple_of(q * quarter + c * CHUNK, CHUNK), CHUNK)

    def o_copy(rel, c, q, target, source):
        return pltpu.make_async_remote_copy(
            source, r_hbm.at[:, out_cols(q, c)], o_send.at[rel, c], o_recv.at[rel, c], **device(target))

    def o_keep(c):
        return pltpu.make_async_copy(r_own.at[:, cols(c)], r_hbm.at[:, out_cols(me, c)], o_local.at[c])

    def finish(c, carry):
        residual(c, GAMMA)
        o_copy(CROSS, c, me, cross, r_own.at[:, cols(c)]).start()
        o_copy(SIB, c, me, sib, r_own.at[:, cols(c)]).start()
        o_keep(c).start()
        return carry

    def relay(c, carry):
        o_copy(CROSS, c, cross, cross, r_own.at[:, cols(c)]).wait_recv()
        o_copy(DIAG, c, cross, sib, r_hbm.at[:, out_cols(cross, c)]).start()
        return carry

    def drain(c, carry):
        o_copy(SIB, c, sib, sib, r_own.at[:, cols(c)]).wait_recv()
        o_copy(DIAG, c, diag, sib, r_own.at[:, cols(c)]).wait_recv()
        for rel, target in ((CROSS, cross), (SIB, sib)):
            o_copy(rel, c, me, target, r_own.at[:, cols(c)]).wait_send()
        o_copy(DIAG, c, cross, sib, r_hbm.at[:, out_cols(cross, c)]).wait_send()
        o_keep(c).wait()
        return carry

    lax.fori_loop(0, steps, finish, 0)
    lax.fori_loop(0, steps, relay, 0)
    lax.fori_loop(0, steps, wait_u, 0)
    lax.fori_loop(0, steps, drain, 0)


def solution(mesh):
    group = mesh.shape['feat']

    def per_device(design, w_init, targets):
        samples, features = design.shape
        labels = w_init.shape[1]
        quarter = samples // group
        steps = quarter // CHUNK
        blocks = features // BLOCK
        vmem = pl.BlockSpec(memory_space=pltpu.VMEM)
        anywhere = pl.BlockSpec(memory_space=pl.ANY)
        dma = pltpu.SemaphoreType.DMA
        weights, residual = pl.pallas_call(
            functools.partial(kernel, samples, group),
            out_shape=(jax.ShapeDtypeStruct((labels, features), F32),
                       jax.ShapeDtypeStruct((labels, samples), F32)),
            in_specs=[anywhere, anywhere, anywhere],
            out_specs=(vmem, anywhere),
            scratch_shapes=[
                pltpu.VMEM((RING, CHUNK, features), BF16),
                pltpu.VMEM((features, CHUNK), BF16),
                pltpu.VMEM((features, CHUNK), BF16),
                pltpu.VMEM((blocks * (blocks + 1) // 2, BLOCK, BLOCK), F32),
                pltpu.VMEM((features, features), BF16),
                pltpu.VMEM((features, features), BF16),
                pltpu.VMEM((1, features), F32),
                pltpu.VMEM((labels, features), BF16),
                pltpu.VMEM((labels, features), F32),
                pltpu.VMEM((labels, quarter), F32),
                pltpu.VMEM((group, labels, quarter), BF16),
                pltpu.VMEM((labels, quarter), BF16),
                pltpu.VMEM((3, labels, quarter), BF16),
                pltpu.VMEM((3, labels, quarter), BF16),
                dma((RING,)),
                dma((3, steps)), dma((3, steps)),
                dma((3, steps)), dma((3, steps)),
                dma((3, steps)), dma((3, steps)),
                dma((steps,)), dma((2,)),
            ],
            compiler_params=pltpu.CompilerParams(
                collective_id=0, has_side_effects=True, vmem_limit_bytes=67000000),
        )(design, w_init.T, targets.T)
        return weights.T, residual.T

    return jax.shard_map(
        per_device,
        mesh=mesh,
        in_specs=(P(None, ('prob', 'feat')), P(('prob', 'feat'), None), P('prob', None)),
        out_specs=(P(('prob', 'feat'), None), P('prob', None)),
        check_vma=False,
    )
```

```python
import functools

import jax
import jax.numpy as jnp
from jax import lax
from jax.experimental import pallas as pl
from jax.experimental.pallas import tpu as pltpu
from jax.sharding import PartitionSpec as P

LOCAL_STEPS = 2
SWEEPS = 6
RIDGE = 0.01
GAMMA = 0.75

MESH = pl.DeviceIdType.MESH
F32 = jnp.float32
BF16 = jnp.bfloat16
CHUNK = 512
RING = 8
BLOCK = 512
HALF = BLOCK // 2
SIB, CROSS, DIAG = 0, 1, 2


def dot(a, b, dims=((1,), (0,))):
    return lax.dot_general(a, b, (dims, ((), ())), preferred_element_type=F32)


MAIN = 96
LANES = 128
PACKED = 4 * MAIN + 24


def pack(ref, value, tail_ref):
    tail_ref[0:value.shape[0] - MAIN, :] = value[MAIN:]
    for g in range(4):
        ref[g * MAIN:(g + 1) * MAIN, :] = value[:MAIN, g * LANES:(g + 1) * LANES].astype(BF16)
    part = [tail_ref[:, g * LANES:(g + 1) * LANES] for g in range(4)]
    row = lax.broadcasted_iota(jnp.int32, part[0].shape, 0)
    first = jnp.where(row < 5, part[0], pltpu.roll(part[3], 5, 0))
    second = jnp.where(row < 5, part[1], pltpu.roll(part[3], 2, 0))
    ref[4 * MAIN:PACKED, :] = jnp.concatenate([first, second, part[2]], axis=0).astype(BF16)


def unpack(ref):
    main = jnp.concatenate([ref[g * MAIN:(g + 1) * MAIN, :] for g in range(4)], axis=1)
    rest = ref[4 * MAIN:PACKED, :].astype(F32)
    part = [rest[8 * g:8 * (g + 1)] for g in range(3)]
    row = lax.broadcasted_iota(jnp.int32, part[0].shape, 0)
    last = jnp.where(row < 3, pltpu.roll(part[0], 3, 0), pltpu.roll(part[1], 6, 0))
    tail = jnp.concatenate(part + [last], axis=1)
    return main, tail


def kernel(samples, group, x_hbm, w0_hbm, y_hbm, w_ref, r_hbm,
           xbuf, xt0, xt1, gram, gram_hi, gram_lo, eta_ref, coef, grad, r_own, r_all, u_mine, u_out, u_in, tail_ref,
           x_sem, u_send, u_recv, r_send, r_recv, o_send, o_recv, o_local, in_sem):
    prob, me = lax.axis_index("prob"), lax.axis_index("feat")
    odd, half = lax.rem(me, 2), me // 2
    sib = half * 2 + (1 - odd)
    cross = (1 - half) * 2 + odd
    diag = (1 - half) * 2 + (1 - odd)
    partner = {SIB: sib, CROSS: cross, DIAG: diag}
    features = x_hbm.shape[1]
    quarter = samples // group
    steps = quarter // CHUNK
    blocks = features // BLOCK

    def device(index):
        return dict(device_id=(prob, index), device_id_type=MESH)

    barrier = pltpu.get_barrier_semaphore()
    for index in (sib, cross, diag):
        pl.semaphore_signal(barrier, inc=1, **device(index))

    def cols(c):
        return pl.ds(pl.multiple_of(c * CHUNK, CHUNK), CHUNK)

    def load(q, c, slot):
        rows = pl.ds(pl.multiple_of(q * quarter + c * CHUNK, CHUNK), CHUNK)
        return pltpu.make_async_copy(x_hbm.at[rows], xbuf.at[slot], x_sem.at[slot])

    a_order = (cross, diag, sib, me)
    b_order = (me, sib)
    c_order = (cross, diag)
    per = {"a": RING // 4, "b": RING // 2, "c": RING // 2}
    orders = {"a": a_order, "b": b_order, "c": c_order}

    def prefetch(phase, c, i, slot):
        load(orders[phase][i], c, slot).start()

    def rounds(phase, nxt, body, together=1):
        n, order = per[phase], orders[phase]
        width = len(order)

        def run(c, ahead):
            for first in range(0, width, together):
                some = range(first, first + together)
                slots = [lax.rem(c * width + i, RING) for i in some]
                for i, slot in zip(some, slots):
                    load(order[i], c, slot).wait()
                sends = [body(c, i, order[i], xbuf.at[slot]) for i, slot in zip(some, slots)]
                for i, slot, send in zip(some, slots, sends):
                    if send is not None:
                        send.start()
                    ahead(c, i, slot)

        def main(c, carry):
            run(c, lambda c, i, slot: prefetch(phase, c + n, i, slot))
            return carry

        def tail(c, carry):
            def ahead(c, i, slot):
                if nxt is None:
                    return
                k = (c - (steps - n)) * width + i
                if nxt == "start":
                    load(diag, k, slot).start()
                elif len(orders[nxt]) == width:
                    prefetch(nxt, c - (steps - n), i, slot)
                elif width == 4:
                    prefetch(nxt, (c - (steps - n)) * 2 + i // 2, i % 2, slot)
                else:
                    j = lax.rem(c - (steps - n), 2)
                    lo, hi = orders[nxt][i], orders[nxt][2 + i]
                    load(lo + j * (hi - lo), (c - (steps - n)) // 2, slot).start()
            run(c, ahead)
            return carry

        lax.fori_loop(0, steps - n, main, 0)
        lax.fori_loop(steps - n, steps, tail, 0)

    def u_copy(rel, c):
        return pltpu.make_async_remote_copy(
            u_out.at[rel, c], u_in.at[rel, c],
            u_send.at[rel, c], u_recv.at[rel, c], **device(partner[rel]))

    def r_copy(rel, c, q, target):
        return pltpu.make_async_remote_copy(
            r_all.at[q, c], r_all.at[q, c],
            r_send.at[rel, c], r_recv.at[rel, c], **device(target))

    a_rel = (CROSS, DIAG, SIB, None)

    def phase_a(nxt, together=1):
        def body(c, i, q, x):
            u = dot(coef[...], x[...], ((1,), (1,)))
            if a_rel[i] is None:
                u_mine[:, cols(c)] = u.astype(BF16)
                return None
            pack(u_out.at[a_rel[i], c], u, tail_ref)
            return u_copy(a_rel[i], c)
        rounds("a", nxt, body, together)

    def residual(c, factor):
        for rel in (SIB, CROSS, DIAG):
            u_copy(rel, c).wait_recv()
        total = u_mine[:, cols(c)].astype(F32)
        for rel in (SIB, CROSS, DIAG):
            main, tail = unpack(u_in.at[rel, c])
            both = jnp.concatenate([main.astype(F32), tail], axis=0)
            total = total + both[:total.shape[0]]
        new = r_own[:, cols(c)] - factor * total
        r_own[:, cols(c)] = new
        return new

    def update(c, factor):
        pack(r_all.at[me, c], residual(c, factor), tail_ref)
        r_copy(CROSS, c, me, cross).start()
        r_copy(SIB, c, me, sib).start()

    def residual_lhs(q, c):
        main, tail = unpack(r_all.at[q, c])
        return jnp.concatenate([main.astype(F32), tail], axis=0).astype(BF16)

    def accumulate(c, q, x):
        grad[...] += dot(residual_lhs(q, c), x[...])[:grad.shape[0]]

    def phase_b():
        def body(c, i, q, x):
            if i == 0:
                update(c, GAMMA)
            else:
                r_copy(SIB, c, sib, sib).wait_recv()
            accumulate(c, q, x)
        grad[...] = jnp.zeros_like(grad)
        rounds("b", "c", body)

    def phase_c():
        def body(c, i, q, x):
            if i == 0:
                r_copy(CROSS, c, cross, cross).wait_recv()
                r_copy(DIAG, c, cross, sib).start()
            else:
                r_copy(DIAG, c, diag, sib).wait_recv()
            accumulate(c, q, x)
        rounds("c", "a", body)

    def wait_u(c, carry):
        for rel in (SIB, CROSS, DIAG):
            u_copy(rel, c).wait_send()
        return carry

    def wait_r(c, carry):
        r_copy(CROSS, c, me, cross).wait_send()
        r_copy(SIB, c, me, sib).wait_send()
        return carry

    def wait_relay(c, carry):
        r_copy(DIAG, c, cross, sib).wait_send()
        return carry

    def local_passes():
        eta = eta_ref[...]
        weights = w_ref[...]
        first = eta * (grad[...] * (1.0 / samples) - RIDGE * weights)
        lhs = first.astype(BF16)
        curved = dot(lhs, gram_hi[...]) + dot(lhs, gram_lo[...])
        curved = jnp.where(eta > 0, curved, 0.0)
        gradient = (grad[...] - (4.0 * group) * curved) * (1.0 / samples)
        second = first + eta * (gradient - RIDGE * (weights + first))
        w_ref[...] = weights + GAMMA * second
        coef[...] = second.astype(BF16)

    def block_index(i, j):
        return i * (i + 1) // 2 + j

    def gram_add(left_ref, right_ref):
        for i in range(blocks):
            for j in range(i + 1):
                left = left_ref[i * BLOCK:(i + 1) * BLOCK, :]
                right = right_ref[:, j * BLOCK:(j + 1) * BLOCK]
                if i == j:
                    gram[block_index(i, j), HALF:, :] += dot(left[HALF:], right)
                    gram[block_index(i, j), :HALF, :HALF] += dot(left[:HALF], right[:, :HALF])
                else:
                    gram[block_index(i, j)] += dot(left, right)

    def start_order(s):
        flip_half, flip_odd = lax.rem(1 + (s + 1) // 2, 2), lax.rem(s + 1, 2)
        return 2 * (half + flip_half * (1 - 2 * half)) + odd + flip_odd * (1 - 2 * odd)

    def start_quarters(first, last, with_gradient):
        def pair(t, carry):
            s, k = t // (steps // 2), lax.rem(t, steps // 2)
            q = start_order(s)
            pairs = ((xt0, xt1), (xt1, xt0))
            for i in range(2):
                c = 2 * k + i
                ahead = lax.rem(c + 1, RING)
                load(q, ahead, ahead).wait()
                if with_gradient:
                    @pl.when(s == 2)
                    def _():
                        r_copy(SIB, c, sib, sib).wait_recv()

                    @pl.when(s == 3)
                    def _():
                        r_copy(CROSS, c, cross, cross).wait_recv()
                        r_copy(DIAG, c, cross, sib).start()
            for i, (now, later) in enumerate(pairs):
                c = 2 * k + i
                later[...] = xbuf[lax.rem(c + 1, RING)].T
                gram_add(now, xbuf.at[c])
                if with_gradient:
                    accumulate(c, q, xbuf.at[c])
            for i in range(2):
                load(start_order(s + 1), 2 * k + i, 2 * k + i).start()
            return carry
        lax.fori_loop(first * (steps // 2), last * (steps // 2), pair, 0)

    def gram_finish():
        trace = jnp.zeros((1, 1), F32)
        for i in range(blocks):
            for j in range(i + 1):
                block = gram[block_index(i, j)]
                if i == j:
                    corner = jnp.concatenate([block[:HALF, :HALF], block[HALF:, :HALF].T], axis=1)
                    block = jnp.concatenate([corner, block[HALF:]], axis=0)
                    row = lax.broadcasted_iota(jnp.int32, block.shape, 0)
                    col = lax.broadcasted_iota(jnp.int32, block.shape, 1)
                    picked = jnp.where(row == col, block, 0.0)
                    trace = trace + jnp.sum(jnp.sum(picked, axis=0, keepdims=True), axis=1, keepdims=True)
                scaled = block * 0.25
                rows, columns = slice(i * BLOCK, (i + 1) * BLOCK), slice(j * BLOCK, (j + 1) * BLOCK)
                high = scaled.astype(BF16)
                low = (scaled - high.astype(F32)).astype(BF16)
                gram_hi[rows, columns] = high
                gram_lo[rows, columns] = low
                if i != j:
                    gram_hi[columns, rows] = high.T
                    gram_lo[columns, rows] = low.T
        eta_ref[...] = jnp.broadcast_to(samples / (group * trace), eta_ref.shape)

    in_w = pltpu.make_async_copy(w0_hbm, w_ref, in_sem.at[0])
    in_y = pltpu.make_async_copy(
        y_hbm.at[:, pl.ds(pl.multiple_of(me * quarter, quarter), quarter)], r_own, in_sem.at[1])
    in_w.start()
    tail_ref[...] = jnp.zeros_like(tail_ref)
    for k in range(RING):
        load(a_order[k % 4], k // 4, k).start()
    in_y.start()
    gram[...] = jnp.zeros_like(gram)
    grad[...] = jnp.zeros_like(grad)
    in_w.wait()
    coef[...] = w_ref[...].astype(BF16)
    pl.semaphore_wait(barrier, 3)
    phase_a("start", 4)
    in_y.wait()

    def first_update(c, carry):
        update(c, 1.0)
        return carry

    load(diag, 0, 0).wait()
    xt0[...] = xbuf[0].T
    start_quarters(0, 1, False)
    lax.fori_loop(0, steps, first_update, 0)
    start_quarters(1, 4, True)
    gram_finish()
    lax.fori_loop(0, steps, wait_u, 0)
    for k in range(steps // 4):
        some = range(4 * k, 4 * k + 4)
        for c in some:
            if c > 0:
                load(diag, c, c).wait()
            r_copy(DIAG, c, diag, sib).wait_recv()
        total = grad[...]
        for c in some:
            total = total + dot(residual_lhs(diag, c), xbuf[c])[:total.shape[0]]
        grad[...] = total
        for c in some:
            load(a_order[c % 4], c // 4, c).start()
    lax.fori_loop(0, steps, wait_relay, 0)
    local_passes()

    def sweep(t, carry):
        phase_a("b")
        lax.fori_loop(0, steps, wait_r, 0)
        phase_b()
        lax.fori_loop(0, steps, wait_u, 0)
        phase_c()
        lax.fori_loop(0, steps, wait_relay, 0)
        local_passes()
        return carry

    lax.fori_loop(0, SWEEPS - 1, sweep, 0)

    phase_a(None)
    lax.fori_loop(0, steps, wait_r, 0)

    def out_cols(q, c):
        return pl.ds(pl.multiple_of(q * quarter + c * CHUNK, CHUNK), CHUNK)

    def o_copy(rel, c, q, target, source):
        return pltpu.make_async_remote_copy(
            source, r_hbm.at[:, out_cols(q, c)], o_send.at[rel, c], o_recv.at[rel, c], **device(target))

    def o_keep(c):
        return pltpu.make_async_copy(r_own.at[:, cols(c)], r_hbm.at[:, out_cols(me, c)], o_local.at[c])

    def finish(c, carry):
        residual(c, GAMMA)
        o_copy(CROSS, c, me, cross, r_own.at[:, cols(c)]).start()
        o_copy(SIB, c, me, sib, r_own.at[:, cols(c)]).start()
        o_keep(c).start()
        return carry

    def relay(c, carry):
        o_copy(CROSS, c, cross, cross, r_own.at[:, cols(c)]).wait_recv()
        o_copy(DIAG, c, cross, sib, r_hbm.at[:, out_cols(cross, c)]).start()
        return carry

    def drain(c, carry):
        o_copy(SIB, c, sib, sib, r_own.at[:, cols(c)]).wait_recv()
        o_copy(DIAG, c, diag, sib, r_own.at[:, cols(c)]).wait_recv()
        for rel, target in ((CROSS, cross), (SIB, sib)):
            o_copy(rel, c, me, target, r_own.at[:, cols(c)]).wait_send()
        o_copy(DIAG, c, cross, sib, r_hbm.at[:, out_cols(cross, c)]).wait_send()
        o_keep(c).wait()
        return carry

    lax.fori_loop(0, steps, finish, 0)
    lax.fori_loop(0, steps, relay, 0)
    lax.fori_loop(0, steps, wait_u, 0)
    lax.fori_loop(0, steps, drain, 0)


def hand_over(w_in, r_in, w_out, r_out, w_buf, r_buf, in_sem, out_sem):
    pieces = r_buf.shape[0]
    width = r_buf.shape[2]

    def views(k):
        if k == pieces:
            return w_in, w_buf, w_out
        columns = pl.ds(k * width, width)
        return r_in.at[:, columns], r_buf.at[k], r_out.at[:, columns]

    ins, outs = [], []
    for k in range(pieces + 1):
        source, buffer, target = views(k)
        ins.append(pltpu.make_async_copy(source, buffer, in_sem.at[k]))
        outs.append(pltpu.make_async_copy(buffer, target, out_sem.at[k]))
    for copy in ins:
        copy.start()
    for first, second in zip(ins, outs):
        first.wait()
        second.start()
    for copy in outs:
        copy.wait()


def solution(mesh):
    group = mesh.shape['feat']

    def per_device(design, w_init, targets):
        samples, features = design.shape
        labels = w_init.shape[1]
        quarter = samples // group
        steps = quarter // CHUNK
        blocks = features // BLOCK
        vmem = pl.BlockSpec(memory_space=pltpu.VMEM)
        anywhere = pl.BlockSpec(memory_space=pl.ANY)
        dma = pltpu.SemaphoreType.DMA
        weights, residual = pl.pallas_call(
            functools.partial(kernel, samples, group),
            out_shape=(jax.ShapeDtypeStruct((labels, features), F32),
                       jax.ShapeDtypeStruct((labels, samples), F32)),
            in_specs=[anywhere, anywhere, anywhere],
            out_specs=(vmem, anywhere),
            scratch_shapes=[
                pltpu.VMEM((RING, CHUNK, features), BF16),
                pltpu.VMEM((features, CHUNK), BF16),
                pltpu.VMEM((features, CHUNK), BF16),
                pltpu.VMEM((blocks * (blocks + 1) // 2, BLOCK, BLOCK), F32),
                pltpu.VMEM((features, features), BF16),
                pltpu.VMEM((features, features), BF16),
                pltpu.VMEM((1, features), F32),
                pltpu.VMEM((labels, features), BF16),
                pltpu.VMEM((labels, features), F32),
                pltpu.VMEM((labels, quarter), F32),
                pltpu.VMEM((group, steps, PACKED, LANES), BF16),
                pltpu.VMEM((labels, quarter), BF16),
                pltpu.VMEM((3, steps, PACKED, LANES), BF16),
                pltpu.VMEM((3, steps, PACKED, LANES), BF16),
                pltpu.VMEM((8, CHUNK), F32),
                dma((RING,)),
                dma((3, steps)), dma((3, steps)),
                dma((3, steps)), dma((3, steps)),
                dma((3, steps)), dma((3, steps)),
                dma((steps,)), dma((2,)),
            ],
            compiler_params=pltpu.CompilerParams(
                collective_id=0, has_side_effects=True, vmem_limit_bytes=67000000),
        )(design, w_init.T, targets.T)
        pieces = 8
        weights, residual = pl.pallas_call(
            hand_over,
            out_shape=(jax.ShapeDtypeStruct(weights.shape, F32), jax.ShapeDtypeStruct(residual.shape, F32)),
            in_specs=[anywhere, anywhere],
            out_specs=(anywhere, anywhere),
            scratch_shapes=[
                pltpu.VMEM(weights.shape, F32),
                pltpu.VMEM((pieces, labels, samples // pieces), F32),
                dma((pieces + 1,)), dma((pieces + 1,)),
            ],
            compiler_params=pltpu.CompilerParams(vmem_limit_bytes=66000000),
        )(weights, residual)
        return weights.T, residual.T

    return jax.shard_map(
        per_device,
        mesh=mesh,
        in_specs=(P(None, ('prob', 'feat')), P(('prob', 'feat'), None), P('prob', None)),
        out_specs=(P(('prob', 'feat'), None), P('prob', None)),
        check_vma=False,
    )
```

```python
import functools

import jax
import jax.numpy as jnp
from jax import lax
from jax.experimental import pallas as pl
from jax.experimental.pallas import tpu as pltpu
from jax.sharding import PartitionSpec as P

LOCAL_STEPS = 2
SWEEPS = 6
RIDGE = 0.01
GAMMA = 0.75

MESH = pl.DeviceIdType.MESH
F32 = jnp.float32
BF16 = jnp.bfloat16
CHUNK = 512
RING = 8
BLOCK = 512
HALF = BLOCK // 2
SIB, CROSS, DIAG = 0, 1, 2


def dot(a, b, dims=((1,), (0,))):
    return lax.dot_general(a, b, (dims, ((), ())), preferred_element_type=F32)


MAIN = 96
LANES = 128
PACKED = 4 * MAIN + 24


def pack(ref, value, tail_ref):
    tail_ref[0:value.shape[0] - MAIN, :] = value[MAIN:]
    for g in range(4):
        ref[g * MAIN:(g + 1) * MAIN, :] = value[:MAIN, g * LANES:(g + 1) * LANES].astype(BF16)
    part = [tail_ref[:, g * LANES:(g + 1) * LANES] for g in range(4)]
    row = lax.broadcasted_iota(jnp.int32, part[0].shape, 0)
    first = jnp.where(row < 5, part[0], pltpu.roll(part[3], 5, 0))
    second = jnp.where(row < 5, part[1], pltpu.roll(part[3], 2, 0))
    ref[4 * MAIN:PACKED, :] = jnp.concatenate([first, second, part[2]], axis=0).astype(BF16)


def unpack(ref):
    main = jnp.concatenate([ref[g * MAIN:(g + 1) * MAIN, :] for g in range(4)], axis=1)
    rest = ref[4 * MAIN:PACKED, :].astype(F32)
    part = [rest[8 * g:8 * (g + 1)] for g in range(3)]
    row = lax.broadcasted_iota(jnp.int32, part[0].shape, 0)
    last = jnp.where(row < 3, pltpu.roll(part[0], 3, 0), pltpu.roll(part[1], 6, 0))
    tail = jnp.concatenate(part + [last], axis=1)
    return main, tail


def kernel(samples, group, x_hbm, w0_hbm, y_hbm, w_ref, r_hbm,
           xbuf, xt0, xt1, gram, gram_hi, gram_lo, eta_ref, coef, grad, r_own, r_all, u_mine, u_out, u_in, tail_ref,
           x_sem, u_send, u_recv, r_send, r_recv, o_send, o_recv, o_local, in_sem):
    prob, me = lax.axis_index("prob"), lax.axis_index("feat")
    odd, half = lax.rem(me, 2), me // 2
    sib = half * 2 + (1 - odd)
    cross = (1 - half) * 2 + odd
    diag = (1 - half) * 2 + (1 - odd)
    partner = {SIB: sib, CROSS: cross, DIAG: diag}
    features = x_hbm.shape[1]
    quarter = samples // group
    steps = quarter // CHUNK
    blocks = features // BLOCK

    def device(index):
        return dict(device_id=(prob, index), device_id_type=MESH)

    barrier = pltpu.get_barrier_semaphore()
    for index in (sib, cross, diag):
        pl.semaphore_signal(barrier, inc=1, **device(index))

    def cols(c):
        return pl.ds(pl.multiple_of(c * CHUNK, CHUNK), CHUNK)

    def load(q, c, slot):
        rows = pl.ds(pl.multiple_of(q * quarter + c * CHUNK, CHUNK), CHUNK)
        return pltpu.make_async_copy(x_hbm.at[rows], xbuf.at[slot], x_sem.at[slot])

    a_order = (cross, diag, sib, me)
    b_order = (me, sib)
    c_order = (cross, diag)
    per = {"a": RING // 4, "b": RING // 2, "c": RING // 2}
    orders = {"a": a_order, "b": b_order, "c": c_order}

    def prefetch(phase, c, i, slot):
        load(orders[phase][i], c, slot).start()

    def rounds(phase, nxt, body, together=1):
        n, order = per[phase], orders[phase]
        width = len(order)

        def run(c, ahead):
            for first in range(0, width, together):
                some = range(first, first + together)
                slots = [lax.rem(c * width + i, RING) for i in some]
                for i, slot in zip(some, slots):
                    load(order[i], c, slot).wait()
                sends = [body(c, i, order[i], xbuf.at[slot]) for i, slot in zip(some, slots)]
                for i, slot, send in zip(some, slots, sends):
                    if send is not None:
                        send.start()
                    ahead(c, i, slot)

        def main(c, carry):
            run(c, lambda c, i, slot: prefetch(phase, c + n, i, slot))
            return carry

        def tail(c, carry):
            def ahead(c, i, slot):
                if nxt is None:
                    return
                k = (c - (steps - n)) * width + i
                if nxt == "start":
                    load(diag, k, slot).start()
                elif len(orders[nxt]) == width:
                    prefetch(nxt, c - (steps - n), i, slot)
                elif width == 4:
                    prefetch(nxt, (c - (steps - n)) * 2 + i // 2, i % 2, slot)
                else:
                    j = lax.rem(c - (steps - n), 2)
                    lo, hi = orders[nxt][i], orders[nxt][2 + i]
                    load(lo + j * (hi - lo), (c - (steps - n)) // 2, slot).start()
            run(c, ahead)
            return carry

        lax.fori_loop(0, steps - n, main, 0)
        lax.fori_loop(steps - n, steps, tail, 0)

    def u_copy(rel, c):
        return pltpu.make_async_remote_copy(
            u_out.at[rel, c], u_in.at[rel, c],
            u_send.at[rel, c], u_recv.at[rel, c], **device(partner[rel]))

    def r_copy(rel, c, q, target):
        return pltpu.make_async_remote_copy(
            r_all.at[q, c], r_all.at[q, c],
            r_send.at[rel, c], r_recv.at[rel, c], **device(target))

    a_rel = (CROSS, DIAG, SIB, None)

    def phase_a(nxt, together=1):
        def body(c, i, q, x):
            u = dot(coef[...], x[...], ((1,), (1,)))
            if a_rel[i] is None:
                u_mine[:, cols(c)] = u.astype(BF16)
                return None
            pack(u_out.at[a_rel[i], c], u, tail_ref)
            return u_copy(a_rel[i], c)
        rounds("a", nxt, body, together)

    def residual(c, factor):
        for rel in (SIB, CROSS, DIAG):
            u_copy(rel, c).wait_recv()
        total = u_mine[:, cols(c)].astype(F32)
        for rel in (SIB, CROSS, DIAG):
            main, tail = unpack(u_in.at[rel, c])
            both = jnp.concatenate([main.astype(F32), tail], axis=0)
            total = total + both[:total.shape[0]]
        new = r_own[:, cols(c)] - factor * total
        r_own[:, cols(c)] = new
        return new

    def update(c, factor):
        pack(r_all.at[me, c], residual(c, factor), tail_ref)
        r_copy(CROSS, c, me, cross).start()
        r_copy(SIB, c, me, sib).start()

    def residual_lhs(q, c):
        main, tail = unpack(r_all.at[q, c])
        return jnp.concatenate([main.astype(F32), tail], axis=0).astype(BF16)

    def accumulate(c, q, x):
        grad[...] += dot(residual_lhs(q, c), x[...])[:grad.shape[0]]

    def phase_b():
        def body(c, i, q, x):
            if i == 0:
                update(c, GAMMA)
            else:
                r_copy(SIB, c, sib, sib).wait_recv()
            accumulate(c, q, x)
        grad[...] = jnp.zeros_like(grad)
        rounds("b", "c", body)

    def phase_c():
        def body(c, i, q, x):
            if i == 0:
                r_copy(CROSS, c, cross, cross).wait_recv()
                r_copy(DIAG, c, cross, sib).start()
            else:
                r_copy(DIAG, c, diag, sib).wait_recv()
            accumulate(c, q, x)
        rounds("c", "a", body)

    def wait_u(c, carry):
        for rel in (SIB, CROSS, DIAG):
            u_copy(rel, c).wait_send()
        return carry

    def wait_r(c, carry):
        r_copy(CROSS, c, me, cross).wait_send()
        r_copy(SIB, c, me, sib).wait_send()
        return carry

    def wait_relay(c, carry):
        r_copy(DIAG, c, cross, sib).wait_send()
        return carry

    def local_passes():
        eta = eta_ref[...]
        weights = w_ref[...]
        first = eta * (grad[...] * (1.0 / samples) - RIDGE * weights)
        lhs = first.astype(BF16)
        curved = dot(lhs, gram_hi[...]) + dot(lhs, gram_lo[...])
        curved = jnp.where(eta > 0, curved, 0.0)
        gradient = (grad[...] - (4.0 * group) * curved) * (1.0 / samples)
        second = first + eta * (gradient - RIDGE * (weights + first))
        w_ref[...] = weights + GAMMA * second
        coef[...] = second.astype(BF16)

    def block_index(i, j):
        return i * (i + 1) // 2 + j

    def gram_add(left_ref, right_ref):
        for i in range(blocks):
            for j in range(i + 1):
                left = left_ref[i * BLOCK:(i + 1) * BLOCK, :]
                right = right_ref[:, j * BLOCK:(j + 1) * BLOCK]
                if i == j:
                    gram[block_index(i, j), HALF:, :] += dot(left[HALF:], right)
                    gram[block_index(i, j), :HALF, :HALF] += dot(left[:HALF], right[:, :HALF])
                else:
                    gram[block_index(i, j)] += dot(left, right)

    def start_order(s):
        flip_half, flip_odd = lax.rem(1 + (s + 1) // 2, 2), lax.rem(s + 1, 2)
        return 2 * (half + flip_half * (1 - 2 * half)) + odd + flip_odd * (1 - 2 * odd)

    def start_quarters(first, last, with_gradient):
        def pair(t, carry):
            s, k = t // (steps // 2), lax.rem(t, steps // 2)
            q = start_order(s)
            pairs = ((xt0, xt1), (xt1, xt0))
            for i in range(2):
                c = 2 * k + i
                ahead = lax.rem(c + 1, RING)
                load(q, ahead, ahead).wait()
                if with_gradient:
                    @pl.when(s == 2)
                    def _():
                        r_copy(SIB, c, sib, sib).wait_recv()

                    @pl.when(s == 3)
                    def _():
                        r_copy(CROSS, c, cross, cross).wait_recv()
                        r_copy(DIAG, c, cross, sib).start()
            for i, (now, later) in enumerate(pairs):
                c = 2 * k + i
                later[...] = xbuf[lax.rem(c + 1, RING)].T
                gram_add(now, xbuf.at[c])
            if with_gradient:
                both = sum(dot(residual_lhs(q, 2 * k + i), xbuf[2 * k + i]) for i in range(2))
                grad[...] += both[:grad.shape[0]]
            for i in range(2):
                load(start_order(s + 1), 2 * k + i, 2 * k + i).start()
            return carry
        lax.fori_loop(first * (steps // 2), last * (steps // 2), pair, 0)

    def gram_finish():
        trace = jnp.zeros((1, 1), F32)
        for i in range(blocks):
            for j in range(i + 1):
                block = gram[block_index(i, j)]
                if i == j:
                    corner = jnp.concatenate([block[:HALF, :HALF], block[HALF:, :HALF].T], axis=1)
                    block = jnp.concatenate([corner, block[HALF:]], axis=0)
                    row = lax.broadcasted_iota(jnp.int32, block.shape, 0)
                    col = lax.broadcasted_iota(jnp.int32, block.shape, 1)
                    picked = jnp.where(row == col, block, 0.0)
                    trace = trace + jnp.sum(jnp.sum(picked, axis=0, keepdims=True), axis=1, keepdims=True)
                scaled = block * 0.25
                rows, columns = slice(i * BLOCK, (i + 1) * BLOCK), slice(j * BLOCK, (j + 1) * BLOCK)
                high = scaled.astype(BF16)
                low = (scaled - high.astype(F32)).astype(BF16)
                gram_hi[rows, columns] = high
                gram_lo[rows, columns] = low
                if i != j:
                    gram_hi[columns, rows] = high.T
                    gram_lo[columns, rows] = low.T
        eta_ref[...] = jnp.broadcast_to(samples / (group * trace), eta_ref.shape)

    in_w = pltpu.make_async_copy(w0_hbm, w_ref, in_sem.at[0])
    in_y = pltpu.make_async_copy(
        y_hbm.at[:, pl.ds(pl.multiple_of(me * quarter, quarter), quarter)], r_own, in_sem.at[1])
    in_w.start()
    tail_ref[...] = jnp.zeros_like(tail_ref)
    for k in range(RING):
        load(a_order[k % 4], k // 4, k).start()
    in_y.start()
    gram[...] = jnp.zeros_like(gram)
    grad[...] = jnp.zeros_like(grad)
    in_w.wait()
    coef[...] = w_ref[...].astype(BF16)
    pl.semaphore_wait(barrier, 3)
    phase_a("start", 4)
    in_y.wait()

    def first_update(c, carry):
        update(c, 1.0)
        return carry

    load(diag, 0, 0).wait()
    xt0[...] = xbuf[0].T
    start_quarters(0, 1, False)
    lax.fori_loop(0, steps, first_update, 0)
    start_quarters(1, 4, True)
    gram_finish()
    lax.fori_loop(0, steps, wait_u, 0)
    for k in range(steps // 4):
        some = range(4 * k, 4 * k + 4)
        for c in some:
            if c > 0:
                load(diag, c, c).wait()
            r_copy(DIAG, c, diag, sib).wait_recv()
        total = grad[...]
        for c in some:
            total = total + dot(residual_lhs(diag, c), xbuf[c])[:total.shape[0]]
        grad[...] = total
        for c in some:
            load(a_order[c % 4], c // 4, c).start()
    lax.fori_loop(0, steps, wait_relay, 0)
    local_passes()

    def sweep(t, carry):
        phase_a("b")
        lax.fori_loop(0, steps, wait_r, 0)
        phase_b()
        lax.fori_loop(0, steps, wait_u, 0)
        phase_c()
        lax.fori_loop(0, steps, wait_relay, 0)
        local_passes()
        return carry

    lax.fori_loop(0, SWEEPS - 1, sweep, 0)

    phase_a(None)
    lax.fori_loop(0, steps, wait_r, 0)

    def out_cols(q, c):
        return pl.ds(pl.multiple_of(q * quarter + c * CHUNK, CHUNK), CHUNK)

    def o_copy(rel, c, q, target, source):
        return pltpu.make_async_remote_copy(
            source, r_hbm.at[:, out_cols(q, c)], o_send.at[rel, c], o_recv.at[rel, c], **device(target))

    def o_keep(c):
        return pltpu.make_async_copy(r_own.at[:, cols(c)], r_hbm.at[:, out_cols(me, c)], o_local.at[c])

    def finish(c, carry):
        residual(c, GAMMA)
        o_copy(CROSS, c, me, cross, r_own.at[:, cols(c)]).start()
        o_copy(SIB, c, me, sib, r_own.at[:, cols(c)]).start()
        o_keep(c).start()
        return carry

    def relay(c, carry):
        o_copy(CROSS, c, cross, cross, r_own.at[:, cols(c)]).wait_recv()
        o_copy(DIAG, c, cross, sib, r_hbm.at[:, out_cols(cross, c)]).start()
        return carry

    def drain(c, carry):
        o_copy(SIB, c, sib, sib, r_own.at[:, cols(c)]).wait_recv()
        o_copy(DIAG, c, diag, sib, r_own.at[:, cols(c)]).wait_recv()
        for rel, target in ((CROSS, cross), (SIB, sib)):
            o_copy(rel, c, me, target, r_own.at[:, cols(c)]).wait_send()
        o_copy(DIAG, c, cross, sib, r_hbm.at[:, out_cols(cross, c)]).wait_send()
        o_keep(c).wait()
        return carry

    lax.fori_loop(0, steps, finish, 0)
    lax.fori_loop(0, steps, relay, 0)
    lax.fori_loop(0, steps, wait_u, 0)
    lax.fori_loop(0, steps, drain, 0)


def hand_over(w_in, r_in, w_out, r_out, w_buf, r_buf, in_sem, out_sem):
    pieces = r_buf.shape[0]
    width = r_buf.shape[2]

    def views(k):
        if k == pieces:
            return w_in, w_buf, w_out
        columns = pl.ds(k * width, width)
        return r_in.at[:, columns], r_buf.at[k], r_out.at[:, columns]

    ins, outs = [], []
    for k in range(pieces + 1):
        source, buffer, target = views(k)
        ins.append(pltpu.make_async_copy(source, buffer, in_sem.at[k]))
        outs.append(pltpu.make_async_copy(buffer, target, out_sem.at[k]))
    for copy in ins:
        copy.start()
    for first, second in zip(ins, outs):
        first.wait()
        second.start()
    for copy in outs:
        copy.wait()


def solution(mesh):
    group = mesh.shape['feat']

    def per_device(design, w_init, targets):
        samples, features = design.shape
        labels = w_init.shape[1]
        quarter = samples // group
        steps = quarter // CHUNK
        blocks = features // BLOCK
        vmem = pl.BlockSpec(memory_space=pltpu.VMEM)
        anywhere = pl.BlockSpec(memory_space=pl.ANY)
        dma = pltpu.SemaphoreType.DMA
        weights, residual = pl.pallas_call(
            functools.partial(kernel, samples, group),
            out_shape=(jax.ShapeDtypeStruct((labels, features), F32),
                       jax.ShapeDtypeStruct((labels, samples), F32)),
            in_specs=[anywhere, anywhere, anywhere],
            out_specs=(vmem, anywhere),
            scratch_shapes=[
                pltpu.VMEM((RING, CHUNK, features), BF16),
                pltpu.VMEM((features, CHUNK), BF16),
                pltpu.VMEM((features, CHUNK), BF16),
                pltpu.VMEM((blocks * (blocks + 1) // 2, BLOCK, BLOCK), F32),
                pltpu.VMEM((features, features), BF16),
                pltpu.VMEM((features, features), BF16),
                pltpu.VMEM((1, features), F32),
                pltpu.VMEM((labels, features), BF16),
                pltpu.VMEM((labels, features), F32),
                pltpu.VMEM((labels, quarter), F32),
                pltpu.VMEM((group, steps, PACKED, LANES), BF16),
                pltpu.VMEM((labels, quarter), BF16),
                pltpu.VMEM((3, steps, PACKED, LANES), BF16),
                pltpu.VMEM((3, steps, PACKED, LANES), BF16),
                pltpu.VMEM((8, CHUNK), F32),
                dma((RING,)),
                dma((3, steps)), dma((3, steps)),
                dma((3, steps)), dma((3, steps)),
                dma((3, steps)), dma((3, steps)),
                dma((steps,)), dma((2,)),
            ],
            compiler_params=pltpu.CompilerParams(
                collective_id=0, has_side_effects=True, vmem_limit_bytes=67000000),
        )(design, w_init.T, targets.T)
        pieces = 16
        weights, residual = pl.pallas_call(
            hand_over,
            out_shape=(jax.ShapeDtypeStruct(weights.shape, F32), jax.ShapeDtypeStruct(residual.shape, F32)),
            in_specs=[anywhere, anywhere],
            out_specs=(anywhere, anywhere),
            scratch_shapes=[
                pltpu.VMEM(weights.shape, F32),
                pltpu.VMEM((pieces, labels, samples // pieces), F32),
                dma((pieces + 1,)), dma((pieces + 1,)),
            ],
            compiler_params=pltpu.CompilerParams(vmem_limit_bytes=66000000),
        )(weights, residual)
        return weights.T, residual.T

    return jax.shard_map(
        per_device,
        mesh=mesh,
        in_specs=(P(None, ('prob', 'feat')), P(('prob', 'feat'), None), P('prob', None)),
        out_specs=(P(('prob', 'feat'), None), P('prob', None)),
        check_vma=False,
    )
```
